256 devices in a mesh: trial: 2 (over core), bank: 4 (over x), zero: 32 (over z, y).
Axes of the slice: x: 4, y: 4, z: 8, core: 2. Of those that a mesh axis runs over, the one named last changes fastest.
Arguments:
- w_gate: float32 [128, 2048, 1024], P(('trial', 'bank'), 'zero'), parts along dimension 0, may hold values from -0.25 to 0.25
- w_up: float32 [128, 2048, 1024], P(('trial', 'bank'), 'zero'), parts along dimension 0, may hold values from -0.25 to 0.25
- router_weight: float32 [4096, 64], P(('trial', 'zero'), 'bank'), parts along dimension 0, may hold values from -0.125 to 0.125
- router_gain: float32 [4096], P(('trial', 'zero')), parts along dimension 0, may hold values from 0.25 to 1.75
Outputs:
- serve_gate: bfloat16 [128, 2048, 1024], P(('trial', 'bank'), None, 'zero'), parts along dimension 0
- serve_up: bfloat16 [128, 2048, 1024], P(('trial', 'bank'), None, 'zero'), parts along dimension 0
- scale_gate: float32 [128, 1024], P(('trial', 'bank'), 'zero'), parts along dimension 0
- scale_up: float32 [128, 1024], P(('trial', 'bank'), 'zero'), parts along dimension 0
- serve_router: bfloat16 [4096, 64], P('trial'), parts along dimension 0
The draws below stay inside these ranges and needn't reach their ends.
There are 2 independent parts, one for each index of `trial`. The reference program is written for one: setup_inputs(seed, part) draws one part's arguments, and reference() takes and returns one part's arrays. A program takes and returns all parts, laid end to end along the dimension named above; each array names one. Nothing has to cross between parts.
All inputs are finite; a program needn't handle non-finite values. Where the reference program divides by a largest or mean magnitude, that divisor is 1e-20 or more.
Results may differ from the reference program's by a relative error of at most 0.001.
Values may be sent and summed in bfloat16 or wider, within the bound.
No kernel may reach another device: no remote copies, remote signals or barrier semaphores. Data moves between devices by JAX's collectives and lax.ppermute only.
A program may use at most 128 MiB of HBM per device.

```python
import jax
import jax.numpy as jnp

EXPERTS = 64
D_MODEL = 2048
D_EXPERT = 1024


def spiked(drawn, key, source, target, parts, factor):
    def block_of(position):
        return (jnp.arange(drawn.shape[position]) // (drawn.shape[position] // parts)).reshape((-1,) + (1,) * (drawn.ndim - 1 - position))

    near = jax.random.permutation(key, parts)[block_of(target)]
    other_side = (block_of(target) + parts // 2) % parts
    return jnp.where((block_of(source) == near) | (block_of(source) == other_side), factor * drawn, drawn)


def level_of(stream_key, dims, cuts, least, top_value):
    def one(dim, parts):
        heights = jax.random.uniform(jax.random.fold_in(jax.random.fold_in(stream_key, 6), dim), (parts,), jnp.float32, least / len(cuts), top_value / len(cuts))
        return jnp.repeat(jnp.exp(heights), dims[dim] // parts).reshape((-1,) + (1,) * (len(dims) - dim - 1))

    gain = one(*cuts[0])
    for cut in cuts[1:]:
        gain = gain * one(*cut)
    return gain


def noise(stream_key, dims, spread, bound, shards=(), held_as=jnp.bfloat16):
    gain = level_of(stream_key, dims, shards, -0.22, 0.18) if shards else 1.0
    entries = jax.random.normal(stream_key, dims, jnp.float32) * spread * gain
    return jnp.minimum(jnp.maximum(entries, -bound), bound).astype(held_as)


def noise_with(rng, extent, width, most, cuts, heavy, kind=jnp.bfloat16):
    array = width * jax.random.normal(rng, extent, jnp.float32)
    if cuts:
        array = array * level_of(rng, extent, cuts, -0.22, 0.18)
    return jnp.clip(spiked(array, jax.random.fold_in(rng, 3), *heavy), -most, most).astype(kind)


def setup_inputs(seed: int = 0, part: int = 0) -> dict:
    arg_keys = jax.random.split(jax.random.key(seed), 5)
    part_splits = jax.random.split(jax.random.fold_in(arg_keys[4], part), 5)
    return {
        "w_gate": noise_with(part_splits[0], (EXPERTS, D_MODEL, D_EXPERT), D_MODEL ** -0.5, 0.25, ((0, 4), (1, 32)), (1, 2, 32, 2.75), jnp.float32),
        "w_up": noise_with(part_splits[1], (EXPERTS, D_MODEL, D_EXPERT), D_MODEL ** -0.5, 0.25, ((0, 4), (1, 32)), (1, 2, 32, 2.75), jnp.float32),
        "router_weight": noise(part_splits[2], (D_MODEL, EXPERTS), D_MODEL ** -0.5, 0.125, ((0, 32), (1, 4)), jnp.float32),
        "router_gain": jnp.clip(1.0 + 0.15 * jax.random.normal(part_splits[3], (D_MODEL,), jnp.float32), 0.25, 1.75),
    }


def reference(w_gate, w_up, router_weight, router_gain):
    scale_gate = jnp.sum(jnp.abs(w_gate), axis=1) / D_MODEL
    serve_gate = (w_gate / jnp.expand_dims(scale_gate, 1)).astype(jnp.bfloat16)
    scale_up = jnp.sum(jnp.abs(w_up), axis=1) / D_MODEL
    serve_up = (w_up / jnp.expand_dims(scale_up, 1)).astype(jnp.bfloat16)
    serve_router = (router_weight * router_gain[:, None]).astype(jnp.bfloat16)
    return serve_gate, serve_up, scale_gate, scale_up, serve_router
```

```python
import jax
import jax.numpy as jnp
from jax import lax
from jax.experimental import pallas as pl
from jax.experimental.pallas import tpu as pltpu
from jax.sharding import PartitionSpec as P

D_MODEL = 2048
LANES = 128
SPAN = 250.0
LN2 = 0.6931471805599453


def coded(w):
    size = jnp.abs(w)
    total = jnp.sum(size, axis=0, keepdims=True)
    top = jnp.max(size, axis=0, keepdims=True)
    top = (top * (1 + 2.0**-7)).astype(jnp.bfloat16).astype(jnp.float32)
    per = jnp.where(top > 1e-30, SPAN / jnp.maximum(top, 1e-30), 0.0)
    code = jnp.exp2(size * per - SPAN / 2)
    high = total.astype(jnp.bfloat16).astype(jnp.float32)
    return jnp.where(w < 0, -code, code), top, high, total - high


def encode_kernel(gate_ref, up_ref, out_ref, stats_ref, *, experts, bands):
    e = pl.program_id(0)

    @pl.when(e < experts)
    def _():
        gate, *gate_stats = coded(gate_ref[0])
        up, *up_stats = coded(up_ref[0])
        for k, (g, u) in enumerate(zip(gate_stats, up_stats)):
            stats_ref[pl.ds(2 * k * experts + e, 1)] = g
            stats_ref[pl.ds((2 * k + 1) * experts + e, 1)] = u
        both = jnp.concatenate([gate, up], axis=0)
        for t in range(bands):
            tile = both[:, t * LANES : (t + 1) * LANES].T.astype(jnp.bfloat16)
            for y in range(4):
                out_ref[4 * t + y] = tile[32 * y : 32 * (y + 1)]

    @pl.when(e == experts)
    def _():
        for t in range(bands):
            tile = stats_ref[:, t * LANES : (t + 1) * LANES].T.astype(jnp.bfloat16)
            for y in range(4):
                out_ref[4 * t + y] = tile[32 * y : 32 * (y + 1)]


def encode(w_gate, w_up):
    experts, rows, columns = w_gate.shape
    last = experts - 1
    return pl.pallas_call(
        lambda *refs: encode_kernel(*refs, experts=experts, bands=columns // LANES),
        name="encode",
        grid=(experts + 1,),
        in_specs=[pl.BlockSpec((1, rows, columns), lambda e: (jnp.minimum(e, last), 0, 0))] * 2,
        out_specs=pl.BlockSpec((32, 32, LANES), lambda e: (0, e, 0)),
        out_shape=jax.ShapeDtypeStruct((32, 32 * (experts + 1), LANES), jnp.bfloat16),
        scratch_shapes=[pltpu.VMEM((LANES, columns), jnp.float32)],
        compiler_params=pltpu.CompilerParams(vmem_limit_bytes=60 << 20),
    )(w_gate, w_up)


def decode_kernel(got_ref, stats_ref, gate_ref, up_ref, gate_scale_ref, up_scale_ref, factor_ref, *, experts):
    e = pl.program_id(0)

    @pl.when(e == 0)
    def _():
        stats = stats_ref[...].astype(jnp.float32)
        total = jnp.sum(stats, axis=0)
        total = pltpu.roll(total, LANES - 2 * experts, 1) + pltpu.roll(total, LANES - 4 * experts, 1)
        scale = total / D_MODEL
        factor_ref[...] = stats * (1.0 / (SPAN * LN2)) / scale[None]
        turned = jnp.concatenate([scale] * 4, axis=0).T
        gate_scale_ref[...] = turned[:experts, :32]
        up_scale_ref[...] = turned[experts : 2 * experts, :32]

    left = lax.broadcasted_iota(jnp.int32, (32, LANES), 1) < 64

    def value(s):
        code = got_ref[s].astype(jnp.float32)
        factor = pltpu.roll(factor_ref[s], LANES - e, 1)
        factor = jnp.where(left, factor[:, :1], factor[:, experts : experts + 1])
        size = (jnp.log(jnp.abs(code)) + SPAN / 2 * LN2) * factor
        return jnp.where(code < 0, -size, size)

    for p in range(16):
        one, two = value(2 * p), value(2 * p + 1)
        gate_ref[0, :, p * LANES : (p + 1) * LANES] = jnp.where(left, one, pltpu.roll(two, 64, 1)).astype(jnp.bfloat16)
        up_ref[0, :, p * LANES : (p + 1) * LANES] = jnp.where(left, pltpu.roll(one, 64, 1), two).astype(jnp.bfloat16)


def decode(got, experts):
    out = jax.ShapeDtypeStruct((experts, 32, D_MODEL), jnp.bfloat16)
    scale = jax.ShapeDtypeStruct((experts, 32), jnp.float32)
    return pl.pallas_call(
        lambda *refs: decode_kernel(*refs, experts=experts),
        name="decode",
        grid=(experts,),
        in_specs=[
            pl.BlockSpec((32, 32, LANES), lambda e: (0, e, 0)),
            pl.BlockSpec((32, 32, LANES), lambda e: (0, experts, 0)),
        ],
        out_specs=[pl.BlockSpec((1, 32, D_MODEL), lambda e: (e, 0, 0))] * 2
        + [pl.BlockSpec((experts, 32), lambda e: (0, 0))] * 2,
        out_shape=[out, out, scale, scale],
        scratch_shapes=[pltpu.VMEM((32, 32, LANES), jnp.float32)],
        compiler_params=pltpu.CompilerParams(vmem_limit_bytes=60 << 20),
    )(got, got)


def sent_to_all(array, axis):
    count = lax.axis_size(axis)
    return lax.all_to_all(jnp.broadcast_to(array[None], (count, *array.shape)), axis, 0, 0, tiled=True)


def local(w_gate, w_up, router_weight, router_gain):
    router = (router_weight * router_gain[:, None]).astype(jnp.bfloat16).T
    router = jnp.moveaxis(sent_to_all(router, "zero"), 0, 1).reshape(router.shape[0], D_MODEL)
    router = sent_to_all(router, "bank").reshape(-1, D_MODEL).T
    sent = encode(w_gate, w_up)
    got = lax.all_to_all(sent, "zero", 0, 0, tiled=True)
    gate, up, scale_gate, scale_up = decode(got, w_gate.shape[0])
    return jnp.swapaxes(gate, 1, 2), jnp.swapaxes(up, 1, 2), scale_gate, scale_up, router


def solution(mesh):
    placed = (
        P(("trial", "bank"), "zero", None),
        P(("trial", "bank"), "zero", None),
        P(("trial", "zero"), "bank"),
        P(("trial", "zero")),
    )
    return jax.shard_map(
        local,
        mesh=mesh,
        in_specs=placed,
        out_specs=(
            P(("trial", "bank"), None, "zero"),
            P(("trial", "bank"), None, "zero"),
            P(("trial", "bank"), "zero"),
            P(("trial", "bank"), "zero"),
            P("trial", None),
        ),
        check_vma=False,
    )
```

```python
import jax
import jax.numpy as jnp
from jax import lax
from jax.experimental import pallas as pl
from jax.experimental.pallas import tpu as pltpu
from jax.sharding import PartitionSpec as P

D_MODEL = 2048
LANES = 128
SPAN = 250.0
LN2 = 0.6931471805599453


def coded(w):
    size = jnp.abs(w)
    total = jnp.sum(size, axis=0, keepdims=True)
    top = jnp.max(size, axis=0, keepdims=True)
    top = (top * (1 + 2.0**-7)).astype(jnp.bfloat16).astype(jnp.float32)
    per = jnp.where(top > 1e-30, SPAN / jnp.maximum(top, 1e-30), 0.0)
    code = jnp.exp2(size * per - SPAN / 2)
    high = total.astype(jnp.bfloat16).astype(jnp.float32)
    return jnp.where(w < 0, -code, code), top, high, total - high


def encode_kernel(gate_ref, up_ref, out_ref, stats_ref, *, experts, bands, group):
    step = pl.program_id(0)

    @pl.when(step < experts // group)
    def _():
        def one(i, _):
            e = step * group + i
            row = pl.multiple_of(i * 32, 32)
            kept = []
            for t in range(bands):
                lanes = slice(t * LANES, (t + 1) * LANES)
                gate, *gate_stats = coded(gate_ref[i, :, lanes])
                up, *up_stats = coded(up_ref[i, :, lanes])
                kept.append([v for pair in zip(gate_stats, up_stats) for v in pair])
                tile = jnp.concatenate([gate, up], axis=0).T.astype(jnp.bfloat16)
                for y in range(4):
                    out_ref[4 * t + y, pl.ds(row, 32)] = tile[32 * y : 32 * (y + 1)]
            for k, parts in enumerate(zip(*kept)):
                stats_ref[pl.ds(k * experts + e, 1)] = jnp.concatenate(parts, axis=1)

        lax.fori_loop(0, group, one, None, unroll=UNROLL)

    @pl.when(step == experts // group)
    def _():
        for t in range(bands):
            tile = stats_ref[:, t * LANES : (t + 1) * LANES].T.astype(jnp.bfloat16)
            for y in range(4):
                out_ref[4 * t + y, :32] = tile[32 * y : 32 * (y + 1)]


GROUP = 4
UNROLL = 2


def encode(w_gate, w_up):
    experts, rows, columns = w_gate.shape
    group = GROUP
    last = experts // group - 1
    return pl.pallas_call(
        lambda *refs: encode_kernel(*refs, experts=experts, bands=columns // LANES, group=group),
        name="encode",
        grid=(experts // group + 1,),
        in_specs=[pl.BlockSpec((group, rows, columns), lambda e: (jnp.minimum(e, last), 0, 0))] * 2,
        out_specs=pl.BlockSpec((32, 32 * group, LANES), lambda e: (0, e, 0)),
        out_shape=jax.ShapeDtypeStruct((32, 32 * (experts + 1), LANES), jnp.bfloat16),
        scratch_shapes=[pltpu.VMEM((LANES, columns), jnp.float32)],
        compiler_params=pltpu.CompilerParams(vmem_limit_bytes=60 << 20),
    )(w_gate, w_up)


def decode_kernel(got_ref, stats_ref, gate_ref, up_ref, gate_scale_ref, up_scale_ref, factor_ref, value_ref, *, experts, group):
    step = pl.program_id(0)

    @pl.when(step == 0)
    def _():
        stats = stats_ref[...].astype(jnp.float32)
        total = jnp.sum(stats, axis=0)
        total = pltpu.roll(total, LANES - 2 * experts, 1) + pltpu.roll(total, LANES - 4 * experts, 1)
        scale = total / D_MODEL
        factor_ref[...] = stats * (1.0 / (SPAN * LN2)) / scale[None]
        turned = jnp.concatenate([scale] * 4, axis=0).T
        gate_scale_ref[...] = turned[:experts, :32]
        up_scale_ref[...] = turned[experts : 2 * experts, :32]

    to = lax.broadcasted_iota(jnp.int32, (2 * LANES, 2 * LANES), 1)
    of = lax.broadcasted_iota(jnp.int32, (2 * LANES, 2 * LANES), 0)
    move = of == to % 64 + to // 64 % 2 * LANES + to // LANES * 64
    move = jnp.where(move, 1.0, 0.0).astype(jnp.bfloat16)

    def one(i, _):
        e = step * group + i
        row = pl.multiple_of(i * 32, 32)
        which = jnp.where(lax.broadcasted_iota(jnp.int32, (32, LANES), 1) < 64, e, experts + e)
        for s in range(32):
            code = got_ref[s, pl.ds(row, 32)].astype(jnp.float32)
            factor = jnp.take_along_axis(factor_ref[s], which, axis=1)
            size = (jnp.log(jnp.abs(code)) + SPAN / 2 * LN2) * factor
            value = jnp.where(code < 0, -size, size).astype(jnp.bfloat16)
            value_ref[i, s // 2 * 32 : s // 2 * 32 + 32, s % 2 * LANES : (s % 2 + 1) * LANES] = value
        both = jnp.dot(value_ref[i], move, preferred_element_type=jnp.float32).astype(jnp.bfloat16)
        for p in range(16):
            gate_ref[i, :, p * LANES : (p + 1) * LANES] = both[p * 32 : (p + 1) * 32, :LANES]
            up_ref[i, :, p * LANES : (p + 1) * LANES] = both[p * 32 : (p + 1) * 32, LANES:]

    lax.fori_loop(0, group, one, None, unroll=UNROLL)


def decode(got, experts):
    out = jax.ShapeDtypeStruct((experts, 32, D_MODEL), jnp.bfloat16)
    scale = jax.ShapeDtypeStruct((experts, 32), jnp.float32)
    group = GROUP
    return pl.pallas_call(
        lambda *refs: decode_kernel(*refs, experts=experts, group=group),
        name="decode",
        grid=(experts // group,),
        in_specs=[
            pl.BlockSpec((32, 32 * group, LANES), lambda e: (0, e, 0)),
            pl.BlockSpec((32, 32, LANES), lambda e: (0, experts, 0)),
        ],
        out_specs=[pl.BlockSpec((group, 32, D_MODEL), lambda e: (e, 0, 0))] * 2
        + [pl.BlockSpec((experts, 32), lambda e: (0, 0))] * 2,
        out_shape=[out, out, scale, scale],
        scratch_shapes=[pltpu.VMEM((32, 32, LANES), jnp.float32), pltpu.VMEM((group, 512, 2 * LANES), jnp.bfloat16)],
        compiler_params=pltpu.CompilerParams(vmem_limit_bytes=60 << 20),
    )(got, got)


def sent_to_all(array, axis):
    count = lax.axis_size(axis)
    return lax.all_to_all(jnp.broadcast_to(array[None], (count, *array.shape)), axis, 0, 0, tiled=True)


def joined(array, axis):
    count, me = lax.axis_size(axis), lax.axis_index(axis)
    near = [array] + [lax.ppermute(array, axis, [(s, (s + k) % count) for s in range(count)]) for k in range(1, count)]
    ring = jnp.concatenate((near[::-1] * 2)[: 2 * count - 1])
    return lax.dynamic_slice_in_dim(ring, (count - 1 - me) * len(array), count * len(array))


def local(w_gate, w_up, router_weight, router_gain):
    router = (router_weight * router_gain[:, None]).astype(jnp.bfloat16).T
    router = jnp.moveaxis(sent_to_all(router, "zero"), 0, 1).reshape(router.shape[0], D_MODEL)
    router = joined(router, "bank").T
    sent = encode(w_gate, w_up)
    got = lax.all_to_all(sent, "zero", 0, 0, tiled=True)
    gate, up, scale_gate, scale_up = decode(got, w_gate.shape[0])
    return jnp.swapaxes(gate, 1, 2), jnp.swapaxes(up, 1, 2), scale_gate, scale_up, router


def solution(mesh):
    placed = (
        P(("trial", "bank"), "zero", None),
        P(("trial", "bank"), "zero", None),
        P(("trial", "zero"), "bank"),
        P(("trial", "zero")),
    )
    return jax.shard_map(
        local,
        mesh=mesh,
        in_specs=placed,
        out_specs=(
            P(("trial", "bank"), None, "zero"),
            P(("trial", "bank"), None, "zero"),
            P(("trial", "bank"), "zero"),
            P(("trial", "bank"), "zero"),
            P("trial", None),
        ),
        check_vma=False,
    )
```

```python
import jax
import jax.numpy as jnp
from jax import lax
from jax.experimental import pallas as pl
from jax.experimental.pallas import tpu as pltpu
from jax.sharding import PartitionSpec as P

D_MODEL = 2048
LANES = 128
SPAN = 126.0
LN2 = 0.6931471805599453
GROUP = 4
DEEP, WIDE = 8, 4
ALL = pltpu.CompilerParams(vmem_limit_bytes=60 << 20)
SOME = pltpu.CompilerParams(vmem_limit_bytes=24 << 20)


def measured(w):
    size = jnp.abs(w)
    total = jnp.sum(size, axis=0, keepdims=True)
    top = jnp.max(size, axis=0, keepdims=True)
    return total, (top * (1 + 2.0**-7)).astype(jnp.bfloat16).astype(jnp.float32)


def coded(w, top):
    return jnp.exp2(w * jnp.where(top > 1e-30, SPAN / jnp.maximum(top, 1e-30), 0.0))


def turned(gate, up, gate_top, up_top):
    return jnp.concatenate([coded(gate, gate_top), coded(up, up_top)], axis=0).T.astype(jnp.bfloat16)


def encode_kernel(gate_ref, up_ref, router_ref, gain_ref, out_ref, stats_ref, *, experts, bands):
    step = pl.program_id(0)
    groups = experts // GROUP

    def one(i, code):
        e = step * GROUP + i
        row = pl.multiple_of(i * 32, 32)
        kept = []
        for t in range(bands):
            lanes = slice(t * LANES, (t + 1) * LANES)
            gate, up = gate_ref[i, :, lanes], up_ref[i, :, lanes]
            gate_total, gate_top = measured(gate)
            up_total, up_top = measured(up)
            gate_high, up_high = (v.astype(jnp.bfloat16).astype(jnp.float32) for v in (gate_total, up_total))
            kept.append((gate_top, up_top, gate_high, up_high, gate_total - gate_high, up_total - up_high))
            if code:
                tile = turned(gate, up, gate_top, up_top)
                for y in range(WIDE):
                    out_ref[WIDE * t + y, pl.ds(row, 32)] = tile[32 * y : 32 * (y + 1)]
        for k, parts in enumerate(zip(*kept)):
            stats_ref[pl.ds(k * experts + e, 1)] = jnp.concatenate(parts, axis=1)

    @pl.when(step < groups - 1)
    def _():
        lax.fori_loop(0, GROUP, lambda i, _: one(i, True), None, unroll=2)

    @pl.when(step == groups - 1)
    def _():
        lax.fori_loop(0, GROUP, lambda i, _: one(i, False), None, unroll=2)
        router = (router_ref[...] * gain_ref[...]).astype(jnp.bfloat16).astype(jnp.float32)
        router = jnp.concatenate([router[:, :32], router[:, 32:]], axis=0)
        router = jnp.concatenate([router] * 4, axis=1)
        for t in range(bands):
            stats_ref[6 * experts :, t * LANES : (t + 1) * LANES] = router
        for t in range(bands):
            tile = stats_ref[:, t * LANES : (t + 1) * LANES].T.astype(jnp.bfloat16)
            for y in range(WIDE):
                out_ref[WIDE * t + y, :32] = tile[32 * y : 32 * (y + 1)]


def encode(w_gate, w_up, router, gain):
    experts, rows, columns = w_gate.shape
    groups = experts // GROUP
    return pl.pallas_call(
        lambda *refs: encode_kernel(*refs, experts=experts, bands=columns // LANES),
        name="encode",
        grid=(groups,),
        in_specs=[pl.BlockSpec((GROUP, rows, columns), lambda g: (g, 0, 0))] * 2
        + [pl.BlockSpec(router.shape, lambda g: (0, 0)), pl.BlockSpec(gain.shape, lambda g: (0, 0))],
        out_specs=pl.BlockSpec((32, 32 * GROUP, LANES), lambda g: (0, g, 0)),
        out_shape=jax.ShapeDtypeStruct((32, 32 * (experts - GROUP + 1), LANES), jnp.bfloat16),
        scratch_shapes=[pltpu.VMEM((LANES, columns), jnp.float32)],
        compiler_params=ALL,
    )(w_gate, w_up, router, gain)


def encode_rest_kernel(at_ref, gate_ref, up_ref, out_ref, *, bands):
    z, y = at_ref[0], at_ref[1]

    def one(i, _):
        row = pl.multiple_of(i * 32, 32)
        for t in range(bands):
            lanes = slice(t * LANES, (t + 1) * LANES)
            gate, up = gate_ref[i, :, lanes], up_ref[i, :, lanes]
            tile = turned(gate, up, measured(gate)[1], measured(up)[1])
            for k in range(WIDE):
                to = (k - y) % WIDE * DEEP + (t - z) % DEEP
                out_ref[to, pl.ds(row, 32)] = tile[32 * k : 32 * (k + 1)]

    lax.fori_loop(0, GROUP, one, None, unroll=2)


def encode_rest(at, w_gate, w_up):
    experts, rows, columns = w_gate.shape
    return pl.pallas_call(
        lambda *refs: encode_rest_kernel(*refs, bands=columns // LANES),
        name="encode_rest",
        grid_spec=pltpu.PrefetchScalarGridSpec(
            num_scalar_prefetch=1,
            grid=(1,),
            in_specs=[pl.BlockSpec((GROUP, rows, columns), lambda _, at: (experts // GROUP - 1, 0, 0))] * 2,
            out_specs=pl.BlockSpec((32, 32 * GROUP, LANES), lambda _, at: (0, 0, 0)),
        ),
        out_shape=jax.ShapeDtypeStruct((32, 32 * GROUP, LANES), jnp.bfloat16),
        compiler_params=ALL,
    )(at, w_gate, w_up)


def unpack_kernel(stats_ref, factor_ref, gate_scale_ref, up_scale_ref, router_ref, *, experts):
    stats = stats_ref[...].astype(jnp.float32)
    total = jnp.sum(stats, axis=0)
    total = pltpu.roll(total, LANES - 2 * experts, 1) + pltpu.roll(total, LANES - 4 * experts, 1)
    scale = total / D_MODEL
    lane = lax.broadcasted_iota(jnp.int32, (32, LANES), 1)
    factor_ref[...] = jnp.where(lane < 2 * experts, stats / (SPAN * LN2) / scale, 0.0)
    scale = jnp.concatenate([scale] * 4, axis=0).T
    gate_scale_ref[...] = scale[:experts, :32]
    up_scale_ref[...] = scale[experts : 2 * experts, :32]
    to = lax.broadcasted_iota(jnp.int32, (2 * LANES, 2 * LANES), 1)
    of = lax.broadcasted_iota(jnp.int32, (2 * LANES, 2 * LANES), 0)
    move = jnp.where(of == to % 32 + to // 64 * 32 + to // 32 % 2 * LANES, 1.0, 0.0).astype(jnp.bfloat16)
    for q in range(DEEP):
        part = stats[4 * q : 4 * (q + 1)].reshape(LANES, LANES).T[6 * experts :].astype(jnp.bfloat16)
        part = jnp.concatenate([part[: len(part) // 2], part[len(part) // 2 :]], axis=1)
        part = jnp.dot(part, move, preferred_element_type=jnp.float32)
        router_ref[:, 2 * LANES * q : 2 * LANES * (q + 1)] = part.astype(jnp.bfloat16)


def unpack(got, experts):
    scale = jax.ShapeDtypeStruct((experts, 32), jnp.float32)
    whole = lambda shape: pl.BlockSpec(shape, lambda _: (0,) * len(shape))
    return pl.pallas_call(
        lambda *refs: unpack_kernel(*refs, experts=experts),
        name="unpack",
        grid=(1,),
        in_specs=[pl.BlockSpec((32, 32, LANES), lambda _: (0, experts - GROUP, 0))],
        out_specs=[whole((32, 32, LANES)), whole((experts, 32)), whole((experts, 32)), whole((16, D_MODEL))],
        out_shape=[
            jax.ShapeDtypeStruct((32, 32, LANES), jnp.float32),
            scale,
            scale,
            jax.ShapeDtypeStruct((16, D_MODEL), jnp.bfloat16),
        ],
        compiler_params=SOME,
    )(got)


def decoded(read, factor_ref, gate_ref, up_ref, value_ref, experts, first):
    to = lax.broadcasted_iota(jnp.int32, (2 * LANES, 2 * LANES), 1)
    of = lax.broadcasted_iota(jnp.int32, (2 * LANES, 2 * LANES), 0)
    move = of == to % 64 + to // 64 % 2 * LANES + to // LANES * 64
    move = jnp.where(move, 1.0, 0.0).astype(jnp.bfloat16)

    def one(i, _):
        row = pl.multiple_of(i * 32, 32)
        e = first + i
        which = jnp.where(lax.broadcasted_iota(jnp.int32, (32, LANES), 1) < 64, e, experts + e)
        for s in range(32):
            factor = jnp.take_along_axis(factor_ref[s], which, axis=1)
            value = (jnp.log(read(s, row).astype(jnp.float32)) * factor).astype(jnp.bfloat16)
            value_ref[i, s // 2 * 32 : s // 2 * 32 + 32, s % 2 * LANES : (s % 2 + 1) * LANES] = value
        both = jnp.dot(value_ref[i], move, preferred_element_type=jnp.float32).astype(jnp.bfloat16)
        for p in range(16):
            gate_ref[i, :, p * LANES : (p + 1) * LANES] = both[p * 32 : (p + 1) * 32, :LANES]
            up_ref[i, :, p * LANES : (p + 1) * LANES] = both[p * 32 : (p + 1) * 32, LANES:]

    lax.fori_loop(0, GROUP, one, None, unroll=2)


def decode_kernel(got_ref, factor_ref, gate_ref, up_ref, value_ref, *, experts):
    read = lambda s, row: got_ref[s, pl.ds(row, 32)]
    decoded(read, factor_ref, gate_ref, up_ref, value_ref, experts, pl.program_id(0) * GROUP)


def decode(got, factor, experts):
    out = jax.ShapeDtypeStruct((experts, 32, D_MODEL), jnp.bfloat16)
    return pl.pallas_call(
        lambda *refs: decode_kernel(*refs, experts=experts),
        name="decode",
        grid=(experts // GROUP - 1,),
        in_specs=[
            pl.BlockSpec((32, 32 * GROUP, LANES), lambda g: (0, g, 0)),
            pl.BlockSpec((32, 32, LANES), lambda g: (0, 0, 0)),
        ],
        out_specs=[pl.BlockSpec((GROUP, 32, D_MODEL), lambda g: (g, 0, 0))] * 2,
        out_shape=[out, out],
        scratch_shapes=[pltpu.VMEM((GROUP, 512, 2 * LANES), jnp.bfloat16)],
        compiler_params=SOME,
    )(got, factor)


def decode_rest_kernel(at_ref, *refs, experts):
    parts, (factor_ref, _, _, gate_ref, up_ref, got_ref, value_ref) = refs[:DEEP], refs[DEEP:]
    z, y = at_ref[0], at_ref[1]
    for k, part in enumerate(parts):
        for j in range(WIDE):
            got_ref[(z - k) % DEEP * WIDE + (y - j) % WIDE] = part[j]
    read = lambda s, row: got_ref[s, pl.ds(row, 32)]
    decoded(read, factor_ref, gate_ref, up_ref, value_ref, experts, experts - GROUP)


def decode_rest(at, parts, factor, gate, up):
    experts = gate.shape[0]
    last = experts // GROUP - 1
    return pl.pallas_call(
        lambda *refs: decode_rest_kernel(*refs, experts=experts),
        name="decode_rest",
        grid_spec=pltpu.PrefetchScalarGridSpec(
            num_scalar_prefetch=1,
            grid=(1,),
            in_specs=[pl.BlockSpec(parts[0].shape, lambda _, at: (0, 0, 0))] * DEEP
            + [pl.BlockSpec((32, 32, LANES), lambda _, at: (0, 0, 0))]
            + [pl.BlockSpec(memory_space=pl.ANY)] * 2,
            out_specs=[pl.BlockSpec((GROUP, 32, D_MODEL), lambda _, at: (last, 0, 0))] * 2,
            scratch_shapes=[
                pltpu.VMEM((32, 32 * GROUP, LANES), jnp.bfloat16),
                pltpu.VMEM((GROUP, 512, 2 * LANES), jnp.bfloat16),
            ],
        ),
        out_shape=[jax.ShapeDtypeStruct(gate.shape, gate.dtype)] * 2,
        input_output_aliases={DEEP + 2: 0, DEEP + 3: 1},
        compiler_params=SOME,
    )(at, *parts, factor, gate, up)


def joined(array, axis):
    count, me = lax.axis_size(axis), lax.axis_index(axis)
    near = [array] + [lax.ppermute(array, axis, [(s, (s + k) % count) for s in range(count)]) for k in range(1, count)]
    ring = jnp.concatenate((near[::-1] * 2)[: 2 * count - 1])
    return lax.dynamic_slice_in_dim(ring, (count - 1 - me) * len(array), count * len(array))


def offset(array, deep, wide):
    pairs = []
    for s in range(DEEP * WIDE):
        z, y = divmod(s, WIDE)
        pairs.append((s, (z + deep) % DEEP * WIDE + (y + wide) % WIDE))
    return lax.ppermute(array, "zero", pairs)


def local(w_gate, w_up, router_weight, router_gain):
    experts = w_gate.shape[0]
    me = lax.axis_index("zero")
    at = jnp.stack([me // WIDE, me % WIDE]).astype(jnp.int32)
    sent = encode(w_gate, w_up, router_weight.T, router_gain[None])
    got = lax.all_to_all(sent, "zero", 0, 0, tiled=True)
    rest = encode_rest(at, w_gate, w_up)
    rows = [rest[:DEEP]]
    for k in range(1, WIDE):
        rows.append(offset(rest[DEEP * k : DEEP * (k + 1)], 0, k))
    parts = [jnp.stack([row[k] for row in rows]) for k in range(DEEP)]
    for k in range(1, DEEP):
        parts[k] = offset(parts[k], k, 0)
    factor, scale_gate, scale_up, router = unpack(got, experts)
    gate, up = decode(got, factor, experts)
    router = joined(router, "bank").T
    gate, up = decode_rest(at, parts, factor, gate, up)
    return jnp.swapaxes(gate, 1, 2), jnp.swapaxes(up, 1, 2), scale_gate, scale_up, router


def solution(mesh):
    placed = (
        P(("trial", "bank"), "zero", None),
        P(("trial", "bank"), "zero", None),
        P(("trial", "zero"), "bank"),
        P(("trial", "zero")),
    )
    return jax.shard_map(
        local,
        mesh=mesh,
        in_specs=placed,
        out_specs=(
            P(("trial", "bank"), None, "zero"),
            P(("trial", "bank"), None, "zero"),
            P(("trial", "bank"), "zero"),
            P(("trial", "bank"), "zero"),
            P("trial", None),
        ),
        check_vma=False,
    )
```

```python
import jax
import jax.numpy as jnp
from jax import lax
from jax.experimental import pallas as pl
from jax.experimental.pallas import tpu as pltpu
from jax.sharding import PartitionSpec as P

D_MODEL = 2048
LANES = 128
SPAN = 126.0
STEP = 250.0 / 26.0
LOW = 0.4 * 256
LN2 = 0.6931471805599453
GROUP = 4
DEEP, WIDE = 8, 4
ALL = pltpu.CompilerParams(vmem_limit_bytes=60 << 20)
SOME = pltpu.CompilerParams(vmem_limit_bytes=24 << 20)


def measured(total, top):
    high = total.astype(jnp.bfloat16).astype(jnp.float32)
    some = jnp.maximum(high, 1e-30)
    n = jnp.floor(jnp.log(jnp.maximum(some / jnp.maximum(top * 1.004, 1e-30), 0.9)) * (4 / LN2))
    f = 0.5 + (total - high) / some * LOW
    bound = high * jnp.exp2(n * -0.25)
    per = jnp.where(bound > 1e-30, SPAN / jnp.maximum(bound, 1e-30), 0.0)
    return high, jnp.exp2((n + 1 + f) * STEP - 125), per


def code_group(first, gates, ups, rows_ref, store):
    bands = gates.shape[2] // LANES
    total_ref, top_ref, per_ref = rows_ref.at[0], rows_ref.at[1], rows_ref.at[2]
    for i in range(GROUP):
        for k, array in enumerate((gates, ups)):
            for t in range(bands):
                lanes = slice(t * LANES, (t + 1) * LANES)
                size = jnp.abs(array[first + i, :, lanes])
                total_ref[2 * i + k : 2 * i + k + 1, lanes] = jnp.sum(size, axis=0, keepdims=True)
                top_ref[2 * i + k : 2 * i + k + 1, lanes] = jnp.max(size, axis=0, keepdims=True)
    high, low, per = measured(total_ref[...], top_ref[...])
    if store is not None:
        per_ref[...] = per
        for i in range(GROUP):
            for t in range(bands):
                lanes = slice(t * LANES, (t + 1) * LANES)
                both = [
                    jnp.exp2(array[first + i, :, lanes] * per_ref[2 * i + k : 2 * i + k + 1, lanes])
                    for k, array in enumerate((gates, ups))
                ]
                store(i, t, jnp.concatenate(both, axis=0).T.astype(jnp.bfloat16))
    return high, low


def encode_kernel(gate_ref, up_ref, router_from, gain_from, out_ref, *scratch, bands):
    gates, ups, codes, router_ref, gain_ref, stats_ref, rows_ref, into, small, out = scratch
    experts = gates.shape[0]
    sent = experts - GROUP

    def arrival(e):
        return (
            pltpu.make_async_copy(gate_ref.at[e], gates.at[e], into.at[0, e]),
            pltpu.make_async_copy(up_ref.at[e], ups.at[e], into.at[1, e]),
        )

    def leaving(first, count, k):
        rows = pl.ds(32 * first, count)
        return pltpu.make_async_copy(codes.at[:, rows], out_ref.at[:, rows], out.at[k])

    def group(g, code):
        first = g * GROUP
        for i in range(GROUP):
            for copy in arrival(first + i):
                copy.wait()

        def store(i, t, tile):
            for y in range(WIDE):
                codes[WIDE * t + y, pl.ds(pl.multiple_of((first + i) * 32, 32), 32)] = tile[32 * y : 32 * (y + 1)]

        high, low = code_group(first, gates, ups, rows_ref, store if code else None)
        stats_ref[pl.ds(pl.multiple_of(2 * first, 8), 2 * GROUP)] = high
        stats_ref[pl.ds(pl.multiple_of(2 * experts + 2 * first, 8), 2 * GROUP)] = low
        if code:
            leaving(first, 32 * GROUP, g).start()

    for e in range(experts):
        for copy in arrival(e):
            copy.start()
    parts = (
        pltpu.make_async_copy(router_from, router_ref, small.at[0]),
        pltpu.make_async_copy(gain_from, gain_ref, small.at[1]),
    )
    for copy in parts:
        copy.start()
    lax.fori_loop(0, sent // GROUP, lambda g, _: group(g, True), None)
    group(sent // GROUP, False)
    for copy in parts:
        copy.wait()
    router = (router_ref[...] * gain_ref[...]).astype(jnp.bfloat16).astype(jnp.float32)
    router = jnp.concatenate([router[:8], router[8:]], axis=1).astype(jnp.bfloat16)
    for t in range(bands):
        tile = stats_ref[:, t * LANES : (t + 1) * LANES].T
        for y in range(WIDE):
            part = tile[32 * y : 32 * (y + 1), :64]
            codes[WIDE * t + y, 32 * sent : 32 * sent + 16] = jnp.concatenate([part[:16], part[16:]], axis=1).astype(jnp.bfloat16)
            codes[WIDE * t + y, 32 * sent + 16 :] = router
    leaving(sent, EXTRA, sent // GROUP).start()
    for k in range(sent // GROUP):
        leaving(k * GROUP, 32 * GROUP, k).wait()
    leaving(sent, EXTRA, sent // GROUP).wait()


EXTRA = 24


def encode(w_gate, w_up, router, gain):
    experts, _, columns = w_gate.shape
    sent = experts - GROUP
    shape = (32, 32 * sent + EXTRA, LANES)
    anywhere = pl.BlockSpec(memory_space=pl.ANY)
    return pl.pallas_call(
        lambda *refs: encode_kernel(*refs, bands=columns // LANES),
        name="encode",
        in_specs=[anywhere] * 4,
        out_specs=anywhere,
        out_shape=jax.ShapeDtypeStruct(shape, jnp.bfloat16),
        scratch_shapes=[
            pltpu.VMEM(w_gate.shape, jnp.float32),
            pltpu.VMEM(w_up.shape, jnp.float32),
            pltpu.VMEM(shape, jnp.bfloat16),
            pltpu.VMEM(router.shape, jnp.float32),
            pltpu.VMEM(gain.shape, jnp.float32),
            pltpu.VMEM((LANES, columns), jnp.float32),
            pltpu.VMEM((3, 2 * GROUP, columns), jnp.float32),
            pltpu.SemaphoreType.DMA((2, experts)),
            pltpu.SemaphoreType.DMA((2,)),
            pltpu.SemaphoreType.DMA((sent // GROUP + 1,)),
        ],
        compiler_params=ALL,
    )(w_gate, w_up, router, gain)


def encode_rest_kernel(at_ref, gate_ref, up_ref, out_ref, rows_ref):
    z, y = at_ref[0], at_ref[1]

    def store(i, t, tile):
        for k in range(WIDE):
            to = (k - y) % WIDE * DEEP + (t - z) % DEEP
            out_ref[to, 32 * i : 32 * (i + 1)] = tile[32 * k : 32 * (k + 1)]

    code_group(0, gate_ref, up_ref, rows_ref, store)


def encode_rest(at, w_gate, w_up):
    experts, rows, columns = w_gate.shape
    return pl.pallas_call(
        encode_rest_kernel,
        name="encode_rest",
        grid_spec=pltpu.PrefetchScalarGridSpec(
            num_scalar_prefetch=1,
            grid=(1,),
            in_specs=[pl.BlockSpec((GROUP, rows, columns), lambda _, at: (experts // GROUP - 1, 0, 0))] * 2,
            out_specs=pl.BlockSpec((32, 32 * GROUP, LANES), lambda _, at: (0, 0, 0)),
            scratch_shapes=[pltpu.VMEM((3, 2 * GROUP, columns), jnp.float32)],
        ),
        out_shape=jax.ShapeDtypeStruct((32, 32 * GROUP, LANES), jnp.bfloat16),
        compiler_params=ALL,
    )(at, w_gate, w_up)


def unpack_kernel(extra_ref, factor_ref, scale_ref, router_ref, *, experts):
    extra = extra_ref[...].astype(jnp.float32)
    lane = lax.broadcasted_iota(jnp.int32, (32, LANES), 1)
    scale = jnp.zeros((32, LANES), jnp.float32)
    for s in range(32):
        high = jnp.concatenate([extra[s, :16], pltpu.roll(extra[s, :16], 64, 1)], axis=0)
        low = pltpu.roll(high, LANES - 2 * experts, 1)
        at = (jnp.log(jnp.maximum(low, 1e-38)) * (1 / LN2) + 125) * (1 / STEP)
        n = jnp.floor(at)
        scale += high * (1 + (at - n - 0.5) * (1 / LOW))
        factor_ref[s] = high * jnp.exp2((n - 1) * -0.25) * (1.0 / (SPAN * LN2))
    scale = scale / D_MODEL
    for s in range(32):
        factor_ref[s] = jnp.where(lane < 2 * experts, factor_ref[s] / scale, 0.0)
    scale_ref[...] = jnp.concatenate([scale] * 4, axis=0).T[: 2 * experts, :32]
    left = lax.broadcasted_iota(jnp.int32, (8, LANES), 1) < 64
    for p in range(16):
        one, two = extra[2 * p, 16:], extra[2 * p + 1, 16:]
        both = [jnp.where(left, one, pltpu.roll(two, 64, 1)), jnp.where(left, pltpu.roll(one, 64, 1), two)]
        router_ref[:, p * LANES : (p + 1) * LANES] = jnp.concatenate(both, axis=0).astype(jnp.bfloat16)


def unpack(got, experts):
    whole = lambda shape: pl.BlockSpec(shape, lambda _: (0,) * len(shape))
    return pl.pallas_call(
        lambda *refs: unpack_kernel(*refs, experts=experts),
        name="unpack",
        grid=(1,),
        in_specs=[pl.BlockSpec((32, EXTRA, LANES), lambda _: (0, 32 * (experts - GROUP) // EXTRA, 0))],
        out_specs=[whole((32, 32, LANES)), whole((2 * experts, 32)), whole((16, D_MODEL))],
        out_shape=[
            jax.ShapeDtypeStruct((32, 32, LANES), jnp.float32),
            jax.ShapeDtypeStruct((2 * experts, 32), jnp.float32),
            jax.ShapeDtypeStruct((16, D_MODEL), jnp.bfloat16),
        ],
        compiler_params=SOME,
    )(got)


def decoded(read, factor_ref, gate_ref, up_ref, value_ref, first):
    to = lax.broadcasted_iota(jnp.int32, (2 * LANES, 2 * LANES), 1)
    of = lax.broadcasted_iota(jnp.int32, (2 * LANES, 2 * LANES), 0)
    move = of == to % 64 + to // 64 % 2 * LANES + to // LANES * 64
    move = jnp.where(move, 1.0, 0.0).astype(jnp.bfloat16)

    def one(i, _):
        row = pl.multiple_of(i * 32, 32)
        e = first + i
        which = 2 * e + lax.broadcasted_iota(jnp.int32, (32, LANES), 1) // 64
        for s in range(32):
            factor = jnp.take_along_axis(factor_ref[s], which, axis=1)
            value = (jnp.log(read(s, row).astype(jnp.float32)) * factor).astype(jnp.bfloat16)
            value_ref[i, s // 2 * 32 : s // 2 * 32 + 32, s % 2 * LANES : (s % 2 + 1) * LANES] = value
        both = jnp.dot(value_ref[i], move, preferred_element_type=jnp.float32).astype(jnp.bfloat16)
        for p in range(16):
            gate_ref[i, :, p * LANES : (p + 1) * LANES] = both[p * 32 : (p + 1) * 32, :LANES]
            up_ref[i, :, p * LANES : (p + 1) * LANES] = both[p * 32 : (p + 1) * 32, LANES:]

    lax.fori_loop(0, GROUP, one, None, unroll=2)


def decode_kernel(got_ref, factor_ref, gate_ref, up_ref, value_ref):
    read = lambda s, row: got_ref[s, pl.ds(row, 32)]
    decoded(read, factor_ref, gate_ref, up_ref, value_ref, pl.program_id(0) * GROUP)


def decode(got, factor, experts):
    out = jax.ShapeDtypeStruct((experts, 32, D_MODEL), jnp.bfloat16)
    return pl.pallas_call(
        lambda *refs: decode_kernel(*refs),
        name="decode",
        grid=(experts // GROUP - 1,),
        in_specs=[
            pl.BlockSpec((32, 32 * GROUP, LANES), lambda g: (0, g, 0)),
            pl.BlockSpec((32, 32, LANES), lambda g: (0, 0, 0)),
        ],
        out_specs=[pl.BlockSpec((GROUP, 32, D_MODEL), lambda g: (g, 0, 0))] * 2,
        out_shape=[out, out],
        scratch_shapes=[pltpu.VMEM((GROUP, 512, 2 * LANES), jnp.bfloat16)],
        compiler_params=SOME,
    )(got, factor)


def decode_rest_kernel(at_ref, *refs, experts):
    parts, (factor_ref, _, _, gate_ref, up_ref, got_ref, value_ref) = refs[:DEEP], refs[DEEP:]
    z, y = at_ref[0], at_ref[1]
    for k, part in enumerate(parts):
        for j in range(WIDE):
            got_ref[(z - k) % DEEP * WIDE + (y - j) % WIDE] = part[j]
    read = lambda s, row: got_ref[s, pl.ds(row, 32)]
    decoded(read, factor_ref, gate_ref, up_ref, value_ref, experts - GROUP)


def decode_rest(at, parts, factor, gate, up):
    experts = gate.shape[0]
    last = experts // GROUP - 1
    return pl.pallas_call(
        lambda *refs: decode_rest_kernel(*refs, experts=experts),
        name="decode_rest",
        grid_spec=pltpu.PrefetchScalarGridSpec(
            num_scalar_prefetch=1,
            grid=(1,),
            in_specs=[pl.BlockSpec(parts[0].shape, lambda _, at: (0, 0, 0))] * DEEP
            + [pl.BlockSpec((32, 32, LANES), lambda _, at: (0, 0, 0))]
            + [pl.BlockSpec(memory_space=pl.ANY)] * 2,
            out_specs=[pl.BlockSpec((GROUP, 32, D_MODEL), lambda _, at: (last, 0, 0))] * 2,
            scratch_shapes=[
                pltpu.VMEM((32, 32 * GROUP, LANES), jnp.bfloat16),
                pltpu.VMEM((GROUP, 512, 2 * LANES), jnp.bfloat16),
            ],
        ),
        out_shape=[jax.ShapeDtypeStruct(gate.shape, gate.dtype)] * 2,
        input_output_aliases={DEEP + 2: 0, DEEP + 3: 1},
        compiler_params=SOME,
    )(at, *parts, factor, gate, up)


def joined(array, axis):
    count, me = lax.axis_size(axis), lax.axis_index(axis)
    near = [array] + [lax.ppermute(array, axis, [(s, (s + k) % count) for s in range(count)]) for k in range(1, count)]
    ring = jnp.concatenate((near[::-1] * 2)[: 2 * count - 1])
    return lax.dynamic_slice_in_dim(ring, (count - 1 - me) * len(array), count * len(array))


def offset(array, deep, wide):
    pairs = []
    for s in range(DEEP * WIDE):
        z, y = divmod(s, WIDE)
        pairs.append((s, (z + deep) % DEEP * WIDE + (y + wide) % WIDE))
    return lax.ppermute(array, "zero", pairs)


def local(w_gate, w_up, router_weight, router_gain):
    experts = w_gate.shape[0]
    me = lax.axis_index("zero")
    at = jnp.stack([me // WIDE, me % WIDE]).astype(jnp.int32)
    sent = encode(w_gate, w_up, router_weight.T, router_gain[None])
    got = lax.all_to_all(sent, "zero", 0, 0, tiled=True)
    rest = encode_rest(at, w_gate, w_up)
    rows = [rest[:DEEP]]
    for k in range(1, WIDE):
        rows.append(offset(rest[DEEP * k : DEEP * (k + 1)], 0, k))
    parts = [jnp.stack([row[k] for row in rows]) for k in range(DEEP)]
    for k in range(1, DEEP):
        parts[k] = offset(parts[k], k, 0)
    factor, scale, router = unpack(got, experts)
    gate, up = decode(got, factor, experts)
    router = joined(router, "bank").T
    at, router, scale = lax.optimization_barrier((at, router, scale.reshape(experts, 2, 32).swapaxes(0, 1)))
    gate, up = decode_rest(at, parts, factor, gate, up)
    return jnp.swapaxes(gate, 1, 2), jnp.swapaxes(up, 1, 2), scale[0], scale[1], router


def solution(mesh):
    placed = (
        P(("trial", "bank"), "zero", None),
        P(("trial", "bank"), "zero", None),
        P(("trial", "zero"), "bank"),
        P(("trial", "zero")),
    )
    return jax.shard_map(
        local,
        mesh=mesh,
        in_specs=placed,
        out_specs=(
            P(("trial", "bank"), None, "zero"),
            P(("trial", "bank"), None, "zero"),
            P(("trial", "bank"), "zero"),
            P(("trial", "bank"), "zero"),
            P("trial", None),
        ),
        check_vma=False,
    )
```

```python
import jax
import jax.numpy as jnp
from jax import lax
from jax.experimental import pallas as pl
from jax.experimental.pallas import tpu as pltpu
from jax.sharding import PartitionSpec as P

D_MODEL = 2048
LANES = 128
SPAN = 126.0
STEP = 250.0 / 26.0
LOW = 0.4 * 256
LN2 = 0.6931471805599453
GROUP = 4
DEEP, WIDE = 8, 4
ALL = pltpu.CompilerParams(vmem_limit_bytes=60 << 20)
SOME = pltpu.CompilerParams(vmem_limit_bytes=24 << 20)


def measured(total, top):
    high = total.astype(jnp.bfloat16).astype(jnp.float32)
    some = jnp.maximum(high, 1e-30)
    n = jnp.floor(jnp.log(jnp.maximum(some / jnp.maximum(top * 1.004, 1e-30), 0.9)) * (4 / LN2))
    f = 0.5 + (total - high) / some * LOW
    bound = high * jnp.exp2(n * -0.25)
    per = jnp.where(bound > 1e-30, SPAN / jnp.maximum(bound, 1e-30), 0.0)
    return high, jnp.exp2((n + 1 + f) * STEP - 125), per


def code_group(first, gates, ups, rows_ref, store):
    bands = gates.shape[2] // LANES
    total_ref, top_ref, per_ref = rows_ref.at[0], rows_ref.at[1], rows_ref.at[2]
    for i in range(GROUP):
        for k, array in enumerate((gates, ups)):
            for t in range(bands):
                lanes = slice(t * LANES, (t + 1) * LANES)
                size = jnp.abs(array[first + i, :, lanes])
                total_ref[2 * i + k : 2 * i + k + 1, lanes] = jnp.sum(size, axis=0, keepdims=True)
                top_ref[2 * i + k : 2 * i + k + 1, lanes] = jnp.max(size, axis=0, keepdims=True)
    high, low, per = measured(total_ref[...], top_ref[...])
    if store is not None:
        per_ref[...] = per
        for i in range(GROUP):
            for t in range(bands):
                lanes = slice(t * LANES, (t + 1) * LANES)
                both = [
                    jnp.exp2(array[first + i, :, lanes] * per_ref[2 * i + k : 2 * i + k + 1, lanes])
                    for k, array in enumerate((gates, ups))
                ]
                store(i, t, jnp.concatenate(both, axis=0).T.astype(jnp.bfloat16))
    return high, low


def encode_kernel(gate_ref, up_ref, router_from, gain_from, out_ref, *scratch, bands):
    gates, ups, codes, router_ref, gain_ref, stats_ref, rows_ref, into, small, out = scratch
    experts = gates.shape[0]
    sent = experts - GROUP

    def arrival(e):
        return (
            pltpu.make_async_copy(gate_ref.at[e], gates.at[e], into.at[0, e]),
            pltpu.make_async_copy(up_ref.at[e], ups.at[e], into.at[1, e]),
        )

    def leaving(first, count, k):
        rows = pl.ds(32 * first, count)
        return pltpu.make_async_copy(codes.at[:, rows], out_ref.at[:, rows], out.at[k])

    def group(g, code):
        first = g * GROUP
        for i in range(GROUP):
            for copy in arrival(first + i):
                copy.wait()

        def store(i, t, tile):
            for y in range(WIDE):
                codes[WIDE * t + y, pl.ds(pl.multiple_of((first + i) * 32, 32), 32)] = tile[32 * y : 32 * (y + 1)]

        high, low = code_group(first, gates, ups, rows_ref, store if code else None)
        stats_ref[pl.ds(pl.multiple_of(2 * first, 8), 2 * GROUP)] = high
        stats_ref[pl.ds(pl.multiple_of(2 * experts + 2 * first, 8), 2 * GROUP)] = low
        if code:
            leaving(first, 32 * GROUP, g).start()

    for e in range(experts):
        for copy in arrival(e):
            copy.start()
    parts = (
        pltpu.make_async_copy(router_from, router_ref, small.at[0]),
        pltpu.make_async_copy(gain_from, gain_ref, small.at[1]),
    )
    for copy in parts:
        copy.start()
    lax.fori_loop(0, sent // GROUP, lambda g, _: group(g, True), None)
    group(sent // GROUP, False)
    for copy in parts:
        copy.wait()
    router = (router_ref[...] * gain_ref[...]).astype(jnp.bfloat16).astype(jnp.float32)
    router = jnp.concatenate([router[:8], router[8:]], axis=1).astype(jnp.bfloat16)
    for t in range(bands):
        tile = stats_ref[:, t * LANES : (t + 1) * LANES].T
        for y in range(WIDE):
            part = tile[32 * y : 32 * (y + 1), :64]
            codes[WIDE * t + y, 32 * sent : 32 * sent + 16] = jnp.concatenate([part[:16], part[16:]], axis=1).astype(jnp.bfloat16)
            codes[WIDE * t + y, 32 * sent + 16 :] = router
    leaving(sent, EXTRA, sent // GROUP).start()
    for k in range(sent // GROUP):
        leaving(k * GROUP, 32 * GROUP, k).wait()
    leaving(sent, EXTRA, sent // GROUP).wait()


EXTRA = 24


def encode(w_gate, w_up, router, gain):
    experts, _, columns = w_gate.shape
    sent = experts - GROUP
    shape = (32, 32 * sent + EXTRA, LANES)
    anywhere = pl.BlockSpec(memory_space=pl.ANY)
    return pl.pallas_call(
        lambda *refs: encode_kernel(*refs, bands=columns // LANES),
        name="encode",
        in_specs=[anywhere] * 4,
        out_specs=anywhere,
        out_shape=jax.ShapeDtypeStruct(shape, jnp.bfloat16),
        scratch_shapes=[
            pltpu.VMEM(w_gate.shape, jnp.float32),
            pltpu.VMEM(w_up.shape, jnp.float32),
            pltpu.VMEM(shape, jnp.bfloat16),
            pltpu.VMEM(router.shape, jnp.float32),
            pltpu.VMEM(gain.shape, jnp.float32),
            pltpu.VMEM((LANES, columns), jnp.float32),
            pltpu.VMEM((3, 2 * GROUP, columns), jnp.float32),
            pltpu.SemaphoreType.DMA((2, experts)),
            pltpu.SemaphoreType.DMA((2,)),
            pltpu.SemaphoreType.DMA((sent // GROUP + 1,)),
        ],
        compiler_params=ALL,
    )(w_gate, w_up, router, gain)


def encode_rest_kernel(at_ref, gate_ref, up_ref, out_ref, rows_ref):
    z, y = at_ref[0], at_ref[1]

    def store(i, t, tile):
        for k in range(WIDE):
            to = (k - y) % WIDE * DEEP + (t - z) % DEEP
            out_ref[to, 32 * i : 32 * (i + 1)] = tile[32 * k : 32 * (k + 1)]

    code_group(0, gate_ref, up_ref, rows_ref, store)


def encode_rest(at, w_gate, w_up):
    experts, rows, columns = w_gate.shape
    return pl.pallas_call(
        encode_rest_kernel,
        name="encode_rest",
        grid_spec=pltpu.PrefetchScalarGridSpec(
            num_scalar_prefetch=1,
            grid=(1,),
            in_specs=[pl.BlockSpec((GROUP, rows, columns), lambda _, at: (experts // GROUP - 1, 0, 0))] * 2,
            out_specs=pl.BlockSpec((32, 32 * GROUP, LANES), lambda _, at: (0, 0, 0)),
            scratch_shapes=[pltpu.VMEM((3, 2 * GROUP, columns), jnp.float32)],
        ),
        out_shape=jax.ShapeDtypeStruct((32, 32 * GROUP, LANES), jnp.bfloat16),
        compiler_params=ALL,
    )(at, w_gate, w_up)


def unpack_kernel(extra_ref, factor_ref, gate_scale_ref, up_scale_ref, router_ref, *, experts):
    extra = extra_ref[...].astype(jnp.float32)
    lane = lax.broadcasted_iota(jnp.int32, (32, LANES), 1)
    scale = jnp.zeros((32, LANES), jnp.float32)
    for s in range(32):
        high = jnp.concatenate([extra[s, :16], pltpu.roll(extra[s, :16], 64, 1)], axis=0)
        low = pltpu.roll(high, LANES - 2 * experts, 1)
        at = (jnp.log(jnp.maximum(low, 1e-38)) * (1 / LN2) + 125) * (1 / STEP)
        n = jnp.floor(at)
        scale += high * (1 + (at - n - 0.5) * (1 / LOW))
        factor_ref[s] = high * jnp.exp2((n - 1) * -0.25) * (1.0 / (SPAN * LN2))
    scale = scale / D_MODEL
    for s in range(32):
        factor_ref[s] = jnp.where(lane < 2 * experts, factor_ref[s] / scale, 0.0)
    scale = jnp.take_along_axis(scale, lane % experts * 2 + lane // experts % 2, axis=1)
    scale = jnp.concatenate([scale] * 4, axis=0).T
    gate_scale_ref[...] = scale[:experts, :32]
    up_scale_ref[...] = scale[experts : 2 * experts, :32]
    left = lax.broadcasted_iota(jnp.int32, (8, LANES), 1) < 64
    for p in range(16):
        one, two = extra[2 * p, 16:], extra[2 * p + 1, 16:]
        both = [jnp.where(left, one, pltpu.roll(two, 64, 1)), jnp.where(left, pltpu.roll(one, 64, 1), two)]
        router_ref[:, p * LANES : (p + 1) * LANES] = jnp.concatenate(both, axis=0).astype(jnp.bfloat16)


def unpack(got, experts):
    whole = lambda shape: pl.BlockSpec(shape, lambda _: (0,) * len(shape))
    return pl.pallas_call(
        lambda *refs: unpack_kernel(*refs, experts=experts),
        name="unpack",
        grid=(1,),
        in_specs=[pl.BlockSpec((32, EXTRA, LANES), lambda _: (0, 32 * (experts - GROUP) // EXTRA, 0))],
        out_specs=[whole((32, 32, LANES)), whole((experts, 32)), whole((experts, 32)), whole((16, D_MODEL))],
        out_shape=[
            jax.ShapeDtypeStruct((32, 32, LANES), jnp.float32),
            jax.ShapeDtypeStruct((experts, 32), jnp.float32),
            jax.ShapeDtypeStruct((experts, 32), jnp.float32),
            jax.ShapeDtypeStruct((16, D_MODEL), jnp.bfloat16),
        ],
        compiler_params=SOME,
    )(got)


def lanes_moved():
    to = lax.broadcasted_iota(jnp.int32, (2 * LANES, 2 * LANES), 1)
    of = lax.broadcasted_iota(jnp.int32, (2 * LANES, 2 * LANES), 0)
    move = of == to % 64 + to // 64 % 2 * LANES + to // LANES * 64
    return jnp.where(move, 1.0, 0.0).astype(jnp.bfloat16)


def decoded(read, factor_ref, gate_ref, up_ref, value_ref, first):
    move = lanes_moved()

    def one(i, _):
        row = pl.multiple_of(i * 32, 32)
        e = first + i
        which = 2 * e + lax.broadcasted_iota(jnp.int32, (32, LANES), 1) // 64
        for s in range(32):
            factor = jnp.take_along_axis(factor_ref[s], which, axis=1)
            value = (jnp.log(read(s, row).astype(jnp.float32)) * factor).astype(jnp.bfloat16)
            value_ref[i, s // 2 * 32 : s // 2 * 32 + 32, s % 2 * LANES : (s % 2 + 1) * LANES] = value
        both = jnp.dot(value_ref[i], move, preferred_element_type=jnp.float32).astype(jnp.bfloat16)
        for p in range(16):
            gate_ref[i, :, p * LANES : (p + 1) * LANES] = both[p * 32 : (p + 1) * 32, :LANES]
            up_ref[i, :, p * LANES : (p + 1) * LANES] = both[p * 32 : (p + 1) * 32, LANES:]

    lax.fori_loop(0, GROUP, one, None, unroll=2)


def decode_kernel(got_ref, factor_ref, gate_ref, up_ref, value_ref):
    read = lambda s, row: got_ref[s, pl.ds(row, 32)]
    decoded(read, factor_ref, gate_ref, up_ref, value_ref, pl.program_id(0) * GROUP)


def decode(got, factor, experts):
    out = jax.ShapeDtypeStruct((experts, 32, D_MODEL), jnp.bfloat16)
    return pl.pallas_call(
        lambda *refs: decode_kernel(*refs),
        name="decode",
        grid=(experts // GROUP - 1,),
        in_specs=[
            pl.BlockSpec((32, 32 * GROUP, LANES), lambda g: (0, g, 0)),
            pl.BlockSpec((32, 32, LANES), lambda g: (0, 0, 0)),
        ],
        out_specs=[pl.BlockSpec((GROUP, 32, D_MODEL), lambda g: (g, 0, 0))] * 2,
        out_shape=[out, out],
        scratch_shapes=[pltpu.VMEM((GROUP, 512, 2 * LANES), jnp.bfloat16)],
        compiler_params=SOME,
    )(got, factor)


def decode_rest_kernel(at_ref, *refs, experts):
    parts, (factor_ref, _, _, gate_to, up_to, value_ref, gates, ups, out) = refs[:DEEP], refs[DEEP:]
    z, y = at_ref[0], at_ref[1]
    move = lanes_moved()

    def leaving(i):
        return (
            pltpu.make_async_copy(gates.at[i], gate_to.at[experts - GROUP + i], out.at[0, i]),
            pltpu.make_async_copy(ups.at[i], up_to.at[experts - GROUP + i], out.at[1, i]),
        )

    for i in range(GROUP):
        which = 2 * (experts - GROUP + i) + lax.broadcasted_iota(jnp.int32, (32, LANES), 1) // 64
        for k, part in enumerate(parts):
            deep = (z - k) % DEEP
            for t in range(WIDE):
                code = part[(y - t) % WIDE, 32 * i : 32 * (i + 1)].astype(jnp.float32)
                factor = jnp.take_along_axis(factor_ref[deep * WIDE + t], which, axis=1)
                row = pl.multiple_of((deep * 2 + t // 2) * 32, 32)
                value = (jnp.log(code) * factor).astype(jnp.bfloat16)
                value_ref[i, pl.ds(row, 32), t % 2 * LANES : (t % 2 + 1) * LANES] = value
        both = jnp.dot(value_ref[i], move, preferred_element_type=jnp.float32).astype(jnp.bfloat16)
        for p in range(16):
            gates[i, :, p * LANES : (p + 1) * LANES] = both[p * 32 : (p + 1) * 32, :LANES]
            ups[i, :, p * LANES : (p + 1) * LANES] = both[p * 32 : (p + 1) * 32, LANES:]
        for copy in leaving(i):
            copy.start()
    for i in range(GROUP):
        for copy in leaving(i):
            copy.wait()


def decode_rest(at, parts, factor, gate, up):
    experts = gate.shape[0]
    anywhere = pl.BlockSpec(memory_space=pl.ANY)
    return pl.pallas_call(
        lambda *refs: decode_rest_kernel(*refs, experts=experts),
        name="decode_rest",
        grid_spec=pltpu.PrefetchScalarGridSpec(
            num_scalar_prefetch=1,
            grid=(1,),
            in_specs=[pl.BlockSpec(parts[0].shape, lambda _, at: (0, 0, 0))] * DEEP
            + [pl.BlockSpec((32, 32, LANES), lambda _, at: (0, 0, 0)), anywhere, anywhere],
            out_specs=[anywhere] * 2,
            scratch_shapes=[
                pltpu.VMEM((GROUP, 512, 2 * LANES), jnp.bfloat16),
                pltpu.VMEM((GROUP, 32, D_MODEL), jnp.bfloat16),
                pltpu.VMEM((GROUP, 32, D_MODEL), jnp.bfloat16),
                pltpu.SemaphoreType.DMA((2, GROUP)),
            ],
        ),
        out_shape=[jax.ShapeDtypeStruct(gate.shape, gate.dtype)] * 2,
        input_output_aliases={DEEP + 2: 0, DEEP + 3: 1},
        compiler_params=SOME,
    )(at, *parts, factor, gate, up)


def joined(array, axis):
    count, me = lax.axis_size(axis), lax.axis_index(axis)
    near = [array] + [lax.ppermute(array, axis, [(s, (s + k) % count) for s in range(count)]) for k in range(1, count)]
    ring = jnp.concatenate((near[::-1] * 2)[: 2 * count - 1])
    return lax.dynamic_slice_in_dim(ring, (count - 1 - me) * len(array), count * len(array))


def offset(array, deep, wide):
    pairs = []
    for s in range(DEEP * WIDE):
        z, y = divmod(s, WIDE)
        pairs.append((s, (z + deep) % DEEP * WIDE + (y + wide) % WIDE))
    return lax.ppermute(array, "zero", pairs)


def local(w_gate, w_up, router_weight, router_gain):
    experts = w_gate.shape[0]
    me = lax.axis_index("zero")
    at = jnp.stack([me // WIDE, me % WIDE]).astype(jnp.int32)
    sent = encode(w_gate, w_up, router_weight.T, router_gain[None])
    got = lax.all_to_all(sent, "zero", 0, 0, tiled=True)
    rest = encode_rest(at, w_gate, w_up)
    rows = [rest[:DEEP]]
    for k in range(1, WIDE):
        rows.append(offset(rest[DEEP * k : DEEP * (k + 1)], 0, k))
    parts = [jnp.stack([row[k] for row in rows]) for k in range(DEEP)]
    for k in range(1, DEEP):
        parts[k] = offset(parts[k], k, 0)
    factor, scale_gate, scale_up, router = unpack(got, experts)
    gate, up = decode(got, factor, experts)
    router = joined(router, "bank").T
    at, router = lax.optimization_barrier((at, router))
    gate, up = decode_rest(at, parts, factor, gate, up)
    return jnp.swapaxes(gate, 1, 2), jnp.swapaxes(up, 1, 2), scale_gate, scale_up, router


def solution(mesh):
    placed = (
        P(("trial", "bank"), "zero", None),
        P(("trial", "bank"), "zero", None),
        P(("trial", "zero"), "bank"),
        P(("trial", "zero")),
    )
    return jax.shard_map(
        local,
        mesh=mesh,
        in_specs=placed,
        out_specs=(
            P(("trial", "bank"), None, "zero"),
            P(("trial", "bank"), None, "zero"),
            P(("trial", "bank"), "zero"),
            P(("trial", "bank"), "zero"),
            P("trial", None),
        ),
        check_vma=False,
    )
```
